32 devices in a mesh: gx: 2 (over x), gy: 4 (over z), gz: 4 (over y, core).
Axes of the slice: x: 2, y: 2, z: 4, core: 2. Of those that a mesh axis runs over, the one named last changes fastest.
Arguments:
- conductivity: float32 [16, 32, 1024], P('gx', 'gy', 'gz'), may hold values from 0.1 to 10
- source: float32 [16, 32, 1024], P('gx', 'gy', 'gz'), may hold values from -5 to 5
Outputs:
- solution: float32 [16, 32, 1024], P('gx', 'gy', 'gz')
- residual: float32 [16, 32, 1024], P('gx', 'gy', 'gz')
The draws below stay inside these ranges and needn't reach their ends.
All inputs are finite; a program needn't handle non-finite values.
Results may differ from the reference program's by a relative error of at most 0.0003.
Values sent between devices are 32-bit elements; how exact they have to be, the bound alone decides.
A program may use at most 64 MiB of HBM per device.

```python
import math
import jax
import jax.numpy as jnp

LEVELS = 3
DEGREE = 4
COARSE_DEGREE = 8
NX = 16
NY = 32
NZ = 1024


def draw_source(key, part):
    rough = jnp.clip(jax.random.normal(key, (NX, NY, NZ), jnp.float32), -5.0, 5.0)
    return rough


def levels(stream_key, dims, cuts, smallest, largest):
    def one(position, parts):
        steps = jax.random.uniform(jax.random.fold_in(jax.random.fold_in(stream_key, 6), position), (parts,), jnp.float32, smallest / len(cuts), largest / len(cuts))
        return jnp.repeat(jnp.exp(steps), dims[position] // parts).reshape((-1,) + (1,) * (len(dims) - position - 1))

    factor_of = one(*cuts[0])
    for cut in cuts[1:]:
        factor_of = factor_of * one(*cut)
    return factor_of


def setup_inputs(seed: int = 0) -> dict:
    seeds = jax.random.split(jax.random.key(seed), 3)
    return {
        "conductivity": jnp.clip(jnp.exp(math.log(10.0) - 4.6051702 * jax.random.uniform(seeds[0], (NX, NY, NZ), jnp.float32) ** levels(seeds[0], (NX, NY, NZ), ((0, 2), (1, 4), (2, 4)), -0.2, 0.2)), 0.1, 10.0),
        "source": draw_source(jax.random.fold_in(seeds[2], 71), 0),
    }


weight_table = {1: 14.0 / 30.0, 2: 3.0 / 30.0, 3: 1.0 / 30.0}
neighbour_offsets = [(along_one, along_two, along_three) for along_one in (-1, 0, 1) for along_two in (-1, 0, 1) for along_three in (-1, 0, 1) if (along_one, along_two, along_three) != (0, 0, 0)]
smooth_low = 0.5
coarse_low = 0.03
upper_bound = 2.0


def shifted(padded, offset):
    return padded[1 + offset[0]:padded.shape[0] - 1 + offset[0], 1 + offset[1]:padded.shape[1] - 1 + offset[1], 1 + offset[2]:padded.shape[2] - 1 + offset[2]]


def stencil(field_pad, coeff_pad, spacing):
    centre_field = shifted(field_pad, (0, 0, 0))
    centre_coeff = shifted(coeff_pad, (0, 0, 0))
    total = jnp.zeros(centre_field.shape, jnp.float32)
    for offset in neighbour_offsets:
        weight = weight_table[abs(offset[0]) + abs(offset[1]) + abs(offset[2])]
        total = total + weight * (centre_coeff + shifted(coeff_pad, offset)) * (centre_field - shifted(field_pad, offset))
    return total * (0.5 / spacing)


def diagonal_of(coeff_pad, spacing):
    centre_coeff = shifted(coeff_pad, (0, 0, 0))
    total = jnp.zeros(centre_coeff.shape, jnp.float32)
    for offset in neighbour_offsets:
        weight = weight_table[abs(offset[0]) + abs(offset[1]) + abs(offset[2])]
        total = total + weight * (centre_coeff + shifted(coeff_pad, offset))
    return total * (0.5 / spacing)


def coarsen(values):
    extent = values.shape
    return values.reshape(extent[0] // 2, 2, extent[1] // 2, 2, extent[2] // 2, 2).mean(axis=(1, 3, 5))


def refine(values):
    return jnp.repeat(jnp.repeat(jnp.repeat(values, 2, axis=0), 2, axis=1), 2, axis=2)


def chebyshev_coefs(degree, lower):
    centre = (upper_bound + lower) / 2.0
    half_width = (upper_bound - lower) / 2.0
    ratio_term = centre / half_width
    rho_prev = 1.0 / ratio_term
    weights = []
    for number in range(1, degree):
        rho_next = 1.0 / (2.0 * ratio_term - rho_prev)
        weights.append((rho_next * rho_prev, 2.0 * rho_next / half_width))
        rho_prev = rho_next
    return centre, weights


def smooth(operate, diagonal, right_side, start, degree, lower, final):
    centre, weights = chebyshev_coefs(degree, lower)
    if start is None:
        residual = right_side
    else:
        residual = right_side - operate(start)
    update = residual / (centre * diagonal)
    solution = update if start is None else start + update
    for pair in weights:
        residual = residual - operate(update)
        update = pair[0] * update + pair[1] * residual / diagonal
        solution = solution + update
    if final:
        residual = residual - operate(update)
    return solution, residual


def reference(conductivity, source):
    coeffs = [conductivity]
    for number in range(1, LEVELS):
        coeffs.append(coarsen(coeffs[-1]))

    def cycle(grid_level, right_side):
        spacing = float(4 ** grid_level)
        coeff_pad = jnp.pad(coeffs[grid_level], 1)
        diagonal = diagonal_of(coeff_pad, spacing)

        def operate(field):
            return stencil(jnp.pad(field, 1), coeff_pad, spacing)

        if grid_level == LEVELS - 1:
            return smooth(operate, diagonal, right_side, None, COARSE_DEGREE, coarse_low, False)
        solution, residual = smooth(operate, diagonal, right_side, None, DEGREE, smooth_low, True)
        correction, ignored = cycle(grid_level + 1, coarsen(residual))
        solution = solution + refine(correction)
        return smooth(operate, diagonal, right_side, solution, DEGREE, smooth_low, grid_level == 0)

    return cycle(0, source)
```

```python
import functools

import jax
import jax.numpy as jnp
from jax import lax
from jax.experimental import pallas as pl
from jax.experimental.pallas import tpu as pltpu
from jax.sharding import PartitionSpec as P

LEVELS = 3
DEGREE = 4
COARSE_DEGREE = 8
MESH = pl.DeviceIdType.MESH


weight_table = {1: 14.0 / 30.0, 2: 3.0 / 30.0, 3: 1.0 / 30.0}
neighbour_offsets = [
    (along_one, along_two, along_three)
    for along_one in (-1, 0, 1)
    for along_two in (-1, 0, 1)
    for along_three in (-1, 0, 1)
    if (along_one, along_two, along_three) != (0, 0, 0)
]
smooth_low = 0.5
coarse_low = 0.03
upper_bound = 2.0


def padded_2(block, sides, width):
    for axis, dim in sides:
        count = lax.axis_size(axis)
        forward = [(i, i + 1) for i in range(count - 1)]
        backward = [(target, source) for source, target in forward]
        low = lax.ppermute(
            lax.slice_in_dim(block, block.shape[dim] - width, None, axis=dim), axis, forward
        )
        high = lax.ppermute(lax.slice_in_dim(block, 0, width, axis=dim), axis, backward)
        block = jnp.concatenate([low, block, high], axis=dim)
    return block


def shifted(padded, offset):
    return padded[
        1 + offset[0] : padded.shape[0] - 1 + offset[0],
        1 + offset[1] : padded.shape[1] - 1 + offset[1],
        1 + offset[2] : padded.shape[2] - 1 + offset[2],
    ]


def inner(values, margin):
    return values[
        margin : values.shape[0] - margin,
        margin : values.shape[1] - margin,
        margin : values.shape[2] - margin,
    ]


def stencil(field_pad, coeff_pad, spacing):
    centre_field = shifted(field_pad, (0, 0, 0))
    centre_coeff = shifted(coeff_pad, (0, 0, 0))
    total = jnp.zeros(centre_field.shape, jnp.float32)
    for offset in neighbour_offsets:
        weight = weight_table[abs(offset[0]) + abs(offset[1]) + abs(offset[2])]
        total = total + weight * (centre_coeff + shifted(coeff_pad, offset)) * (
            centre_field - shifted(field_pad, offset)
        )
    return total * (0.5 / spacing)


def diagonal_of(coeff_pad, spacing):
    centre_coeff = shifted(coeff_pad, (0, 0, 0))
    total = jnp.zeros(centre_coeff.shape, jnp.float32)
    for offset in neighbour_offsets:
        weight = weight_table[abs(offset[0]) + abs(offset[1]) + abs(offset[2])]
        total = total + weight * (centre_coeff + shifted(coeff_pad, offset))
    return total * (0.5 / spacing)


def coarsen(values):
    extent = values.shape
    return values.reshape(extent[0] // 2, 2, extent[1] // 2, 2, extent[2] // 2, 2).mean(
        axis=(1, 3, 5)
    )


def refine(values):
    return jnp.repeat(jnp.repeat(jnp.repeat(values, 2, axis=0), 2, axis=1), 2, axis=2)


def chebyshev_coefs(degree, lower):
    centre = (upper_bound + lower) / 2.0
    half_width = (upper_bound - lower) / 2.0
    ratio_term = centre / half_width
    rho_prev = 1.0 / ratio_term
    weights = []
    for number in range(1, degree):
        rho_next = 1.0 / (2.0 * ratio_term - rho_prev)
        weights.append((rho_next * rho_prev, 2.0 * rho_next / half_width))
        rho_prev = rho_next
    return (centre, weights)


def inside_mask(extent, margin):
    first_pos = (
        lax.axis_index("gx") * extent[0]
        + jnp.arange(extent[0] + 2 * margin, dtype=jnp.int32)
        - margin
    )
    second_pos = (
        lax.axis_index("gy") * extent[1]
        + jnp.arange(extent[1] + 2 * margin, dtype=jnp.int32)
        - margin
    )
    third_pos = (
        lax.axis_index("gz") * extent[2]
        + jnp.arange(extent[2] + 2 * margin, dtype=jnp.int32)
        - margin
    )
    first_ok = (first_pos >= 0) & (first_pos < extent[0] * lax.axis_size("gx"))
    second_ok = (second_pos >= 0) & (second_pos < extent[1] * lax.axis_size("gy"))
    third_ok = (third_pos >= 0) & (third_pos < extent[2] * lax.axis_size("gz"))
    return first_ok[:, None, None] & second_ok[None, :, None] & third_ok[None, None, :]


def operate_near(context, field):
    spacing, coeff_ext, diagonal_ext, inside = context
    padded = padded_2(field, (("gx", 0), ("gy", 1), ("gz", 2)), 1)
    return stencil(padded, inner(coeff_ext, 1), spacing)


def two_steps(context, solution, residual, update, first_pair, second_pair):
    spacing, coeff_ext, diagonal_ext, inside = context
    diagonal = inner(diagonal_ext, 1)
    stacked = jnp.stack([update, residual])
    padded = padded_2(stacked, (("gx", 1), ("gy", 2), ("gz", 3)), 2)
    update_wide = padded[0]
    residual_wide = padded[1]
    residual_near = inner(residual_wide, 1) - stencil(update_wide, coeff_ext, spacing)
    update_near = (
        first_pair[0] * inner(update_wide, 1) + first_pair[1] * residual_near / diagonal_ext
    )
    update_near = jnp.where(inside, update_near, 0.0)
    solution = solution + inner(update_near, 1)
    residual = inner(residual_near, 1) - stencil(update_near, inner(coeff_ext, 1), spacing)
    if second_pair is None:
        update = inner(update_near, 1)
    else:
        update = second_pair[0] * inner(update_near, 1) + second_pair[1] * residual / diagonal
        solution = solution + update
    return (solution, residual, update)


def relax(context, right_side, start, degree, lower, final):
    diagonal = inner(context[2], 1)
    centre, weights = chebyshev_coefs(degree, lower)
    if start is None:
        residual = right_side
    else:
        residual = right_side - operate_near(context, start)
    update = residual / (centre * diagonal)
    solution = update if start is None else start + update
    plan_list = list(weights) + ([None] if final else [])
    position = 0
    while position + 1 < len(plan_list):
        solution, residual, update = two_steps(
            context, solution, residual, update, plan_list[position], plan_list[position + 1]
        )
        position = position + 2
    leftover = plan_list[position:]
    for pair in leftover:
        residual = residual - operate_near(context, update)
        update = pair[0] * update + pair[1] * residual / diagonal
        solution = solution + update
    return (solution, residual)


def body(conductivity, source):
    coeff_now = conductivity
    contexts = []
    for grid_level in range(LEVELS):
        if grid_level > 0:
            coeff_now = coarsen(coeff_now)
        spacing = float(4**grid_level)
        coeff_ext = padded_2(coeff_now, (("gx", 0), ("gy", 1), ("gz", 2)), 2)
        inside = inside_mask(coeff_now.shape, 1)
        diagonal_ext = jnp.where(inside, diagonal_of(coeff_ext, spacing), 1.0)
        contexts.append((spacing, coeff_ext, diagonal_ext, inside))

    def cycle(grid_level, right_side):
        context = contexts[grid_level]
        if grid_level == LEVELS - 1:
            return relax(context, right_side, None, COARSE_DEGREE, coarse_low, False)
        solution, residual = relax(context, right_side, None, DEGREE, smooth_low, True)
        correction, ignored = cycle(grid_level + 1, coarsen(residual))
        solution = solution + refine(correction)
        return relax(context, right_side, solution, DEGREE, smooth_low, grid_level == 0)

    return cycle(0, source)


def cells(shape, dim):
    return lax.broadcasted_iota(jnp.int32, shape, dim)


def pick(left, right):
    if left.dtype == jnp.bfloat16:
        dense, other, swap = right, left, False
    else:
        dense, other, swap = left, right, True
    total = None
    for _ in range(3):
        part = dense.astype(jnp.bfloat16)
        dense = dense - part.astype(jnp.float32)
        pair = (part, other) if swap else (other, part)
        term = jnp.dot(*pair, preferred_element_type=jnp.float32)
        total = term if total is None else total + term
    return total


def ones_where(condition):
    return jnp.where(condition, 1.0, 0.0).astype(jnp.bfloat16)


def turn(values, shift, dim):
    return pltpu.roll(values, shift % values.shape[dim], dim)


def pair_sum(values, dim, edges):
    low = turn(values, 1, dim)
    high = turn(values, -1, dim)
    if edges is not None:
        low = jnp.where(edges[dim][0], 0.0, low)
        high = jnp.where(edges[dim][1], 0.0, high)
    return low + high


def plane_sums(values, edges):
    beside = pair_sum(values, 1, edges)
    strong = 14.0 * values + 3.0 * beside
    weak = 3.0 * values + beside
    return pair_sum(strong, 0, edges) + 14.0 * beside, pair_sum(weak, 0, edges) + strong


class Level:
    def __init__(self, refs, scale, wraps):
        self.k, self.r, self.d, self.di, self.dg, self.e, self.f, self.g = refs
        self.scale = scale
        shape = self.k.shape[1:]
        self.edges = None
        if not wraps:
            self.edges = [
                (cells(shape, dim) == 0, cells(shape, dim) == shape[dim] - 1) for dim in (0, 1)
            ]

    def diagonal(self, wide, near, inside):
        def first(p, carry):
            here, side = plane_sums(self.k[p], self.edges)
            self.e[p] = here
            self.g[p] = side
            return carry

        lax.fori_loop(wide[0], wide[1], first, 0)

        def second(p, carry):
            total = 128.0 * self.k[p] + self.e[p] + self.g[p - 1] + self.g[p + 1]
            total = total * self.scale
            self.dg[p] = total
            good = total > 0.0
            if inside is not None:
                good = good & inside
            self.di[p] = jnp.where(good, 1.0 / total, 0.0)
            return carry

        lax.fori_loop(near[0], near[1], second, 0)

    def first_update(self, span, centre):
        def step(p, carry):
            self.d[p] = self.r[p] * self.di[p] * (1.0 / centre)
            return carry

        lax.fori_loop(span[0], span[1], step, 0)

    def apply(self, wide, near, pair):
        def first(p, carry):
            field = self.d[p]
            coeff = self.k[p]
            here, side = plane_sums(field, self.edges)
            here_k, side_k = plane_sums(coeff * field, self.edges)
            self.e[p] = coeff * here + here_k
            self.f[p] = side
            self.g[p] = side_k
            return carry

        lax.fori_loop(wide[0], wide[1], first, 0)

        def second(p, carry):
            field = self.d[p]
            around = self.e[p] + self.k[p] * (self.f[p - 1] + self.f[p + 1])
            around = around + (self.g[p - 1] + self.g[p + 1])
            left = self.r[p] - (self.dg[p] * field - self.scale * around)
            self.r[p] = left
            if pair is not None:
                fresh = pair[1] * (left * self.di[p])
                self.d[p] = fresh if pair[0] == 0.0 else pair[0] * field + fresh
            return carry

        lax.fori_loop(near[0], near[1], second, 0)


def kernel(sizes, block, *refs):
    (nx, ny, nz) = sizes
    (bx, by, bz) = block
    count = nx * ny * nz
    (k_in, b_in, x_out, r_out) = refs[:4]
    fine_refs = refs[4:12]
    mid_refs = refs[12:20]
    low_refs = refs[20:28]
    (far, x_mid, b_mid, x_low) = refs[28:32]
    (k_send, b_send, r_send, k_got, b_got) = refs[32:37]
    (pack_out, pack_in) = refs[37:39]
    (halo_out, halo_in, z_out, z_in, all_out, all_in) = refs[39:45]
    ix, iy, iz = lax.axis_index("gx"), lax.axis_index("gy"), lax.axis_index("gz")
    me = (ix * ny + iy) * nz + iz
    reach = 5

    def place(number):
        return (number // (ny * nz), (number // nz) % ny, number % nz)

    for ref in (*fine_refs, *mid_refs, *low_refs, far):
        def clear(p, carry, ref=ref):
            ref[p] = jnp.zeros(ref.shape[1:], jnp.float32)
            return carry

        lax.fori_loop(0, ref.shape[0], clear, 0)

    barrier = pltpu.get_barrier_semaphore()

    def greet(j, carry):
        pl.semaphore_signal(
            barrier, inc=1, device_id=place((me + j) % count), device_id_type=MESH
        )
        return carry

    lax.fori_loop(1, count, greet, 0)
    pl.semaphore_wait(barrier, count - 1)

    fine = Level(fine_refs, 0.5 / 30.0, True)
    mid = Level(mid_refs, 0.5 / 4.0 / 30.0, False)
    low = Level(low_refs, 0.5 / 16.0 / 30.0, False)

    def near_copy(source, target, which, dx, dy):
        planes = bx if dx == 0 else reach
        first_from = 0 if dx <= 0 else bx - reach
        first_to = {0: bx, 1: bx - reach, -1: 2 * bx}[dx]
        row_to = {0: 0, 1: 2 * by, -1: by}[dy]
        number = (dx + 1) * 3 + dy + 1
        return pltpu.make_async_remote_copy(
            src_ref=source.at[pl.ds(first_from, planes)],
            dst_ref=target.at[pl.ds(first_to, planes), pl.ds(row_to, by), pl.ds(0, bz)],
            send_sem=halo_out.at[which, number],
            recv_sem=halo_in.at[which, number],
            device_id=(ix + dx, iy + dy, iz),
            device_id_type=MESH,
        )

    sides = [(dx, dy) for dx in (0, 1, -1) for dy in (1, -1, 0) if (dx, dy) != (0, 0)]

    def present(dx, dy):
        return (ix + dx >= 0) & (ix + dx < nx) & (iy + dy >= 0) & (iy + dy < ny)

    def near_start(source, target, which):
        for dx, dy in sides:
            @pl.when(present(dx, dy))
            def _():
                near_copy(source, target, which, dx, dy).start()

    def near_wait(source, target, which):
        for dx, dy in sides:
            @pl.when(present(-dx, -dy))
            def _():
                near_copy(source, target, which, dx, dy).wait_recv()

            @pl.when(present(dx, dy))
            def _():
                near_copy(source, target, which, dx, dy).wait_send()

    lane = cells((3 * by, 128), 1)
    z_planes = list(range(bx - reach, 2 * bx + reach))
    groups = (len(z_planes) + 15) // 16

    def z_copy(which, side):
        return pltpu.make_async_remote_copy(
            src_ref=pack_out.at[which, side],
            dst_ref=pack_in.at[which, side],
            send_sem=z_out.at[which, side],
            recv_sem=z_in.at[which, side],
            device_id=(ix, iy, iz + (1 if side == 0 else -1)),
            device_id_type=MESH,
        )

    to_there = (iz + 1 < nz, iz > 0)
    from_there = (iz > 0, iz + 1 < nz)

    def z_start(window, which):
        for group in range(groups):
            up = jnp.zeros((3 * by, 128), jnp.float32)
            down = jnp.zeros((3 * by, 128), jnp.float32)
            for i, p in enumerate(z_planes[group * 16 : group * 16 + 16]):
                mine = lane // 8 == i
                up = jnp.where(mine, turn(window[p, :, bz - 128 : bz], 8 * i + 8, 1), up)
                down = jnp.where(mine, turn(window[p, :, 0:128], 8 * i, 1), down)
            pack_out[which, 0, group] = up
            pack_out[which, 1, group] = down
        for side in (0, 1):
            @pl.when(to_there[side])
            def _():
                z_copy(which, side).start()

    def z_finish(window, which):
        for side in (0, 1):
            @pl.when(from_there[side])
            def _():
                z_copy(which, side).wait_recv()

            @pl.when(jnp.logical_not(from_there[side]))
            def _():
                pack_in[which, side] = jnp.zeros(pack_in.shape[2:], jnp.float32)

            @pl.when(to_there[side])
            def _():
                z_copy(which, side).wait_send()

        for group in range(groups):
            below = pack_in[which, 0, group]
            above = pack_in[which, 1, group]
            for i, p in enumerate(z_planes[group * 16 : group * 16 + 16]):
                window[p, :, bz : bz + 128] = jnp.where(
                    lane < 64, turn(above, -8 * i, 1), turn(below, -8 * i - 8, 1)
                )

    def all_copy(source, target, which, peer, slot):
        return pltpu.make_async_remote_copy(
            src_ref=source,
            dst_ref=target.at[slot],
            send_sem=all_out.at[which, peer],
            recv_sem=all_in.at[which, slot],
            device_id=place(peer),
            device_id_type=MESH,
        )

    def all_start(source, target, which):
        target[me] = source[...]

        def step(j, carry):
            all_copy(source, target, which, (me + j) % count, me).start()
            return carry

        lax.fori_loop(1, count, step, 0)

    def all_wait(source, target, which):
        def step(j, carry):
            peer = (me + j) % count
            all_copy(source, target, which, peer, peer).wait_recv()
            all_copy(source, target, which, peer, me).wait_send()
            return carry

        lax.fori_loop(1, count, step, 0)

    half = bx // 2 * (by // 2)
    to_row, from_row = cells((half, bx * by), 0), cells((half, bx * by), 1)
    shrink = ones_where(
        (from_row // by // 2 == to_row // (by // 2)) & (from_row % by // 2 == to_row % (by // 2))
    )
    shrink_z = ones_where(cells((bz, bz // 2), 0) // 2 == cells((bz, bz // 2), 1))

    def coarse_block(values):
        flat = pick(pick(shrink, values.reshape(bx * by, bz)), shrink_z) * 0.125
        return flat.reshape(half // 8, 8, bz // 2)

    row8 = cells((8, bz // 2), 0)

    def unpack(got, target):
        for jx in range(nx):
            for jy in range(0, ny, 2):
                for jz in range(nz):
                    slot = (jx * ny + jy) * nz + jz
                    for t in range(half // 8):
                        one, two = got[slot, t], got[slot + nz, t]
                        p = 1 + jx * (bx // 2) + 2 * t
                        at = (slice(jy * 4, jy * 4 + 8), slice(jz * bz // 2, (jz + 1) * bz // 2))
                        target[(p, *at)] = jnp.where(row8 < 4, one, turn(two, 4, 0))
                        target[(p + 1, *at)] = jnp.where(row8 < 4, turn(one, 4, 0), two)

    near_start(k_in, fine.k, 0)
    near_start(b_in, fine.r, 1)
    k_send[...] = coarse_block(k_in[...])
    all_start(k_send, k_got, 0)
    fine.k[bx : 2 * bx, 0:by, 0:bz] = k_in[...]
    fine.r[bx : 2 * bx, 0:by, 0:bz] = b_in[...]
    near_wait(k_in, fine.k, 0)
    z_start(fine.k, 0)
    near_wait(b_in, fine.r, 1)
    z_start(fine.r, 1)
    z_finish(fine.k, 0)

    def span(width):
        return (
            jnp.maximum(bx - width, bx - ix * bx),
            jnp.minimum(2 * bx + width, bx + (nx - ix) * bx),
        )

    plane = (3 * by, bz + 128)
    row, col = cells(plane, 0), cells(plane, 1)
    inside = (
        (row < by) | ((row < 2 * by) & (iy + 1 < ny)) | ((row >= 2 * by) & (iy > 0))
    ) & ((col < bz) | ((col < bz + 64) & (iz + 1 < nz)) | ((col >= bz + 64) & (iz > 0)))
    fine.diagonal(span(5), span(4), inside)
    z_finish(fine.r, 1)

    own = (slice(bx, 2 * bx), slice(0, by), slice(0, bz))
    centre, weights = chebyshev_coefs(DEGREE, smooth_low)
    fine.first_update(span(4), centre)
    x_out[...] = fine.d[own]
    for number in range(DEGREE):
        pair = weights[number] if number < DEGREE - 1 else None
        fine.apply(span(4 - number), span(3 - number), pair)
        if pair is not None:
            x_out[...] += fine.d[own]

    r_send[...] = fine.r[own]
    b_send[...] = coarse_block(r_send[...])
    all_start(b_send, b_got, 1)
    near_start(r_send, far, 2)
    far[own] = r_send[...]

    mx, my, mz = mid.k.shape[0] - 2, mid.k.shape[1], mid.k.shape[2]
    cx, cy, cz = mx // 2, my // 2, mz // 2
    mid_span, low_span = (1, mx + 1), (1, cx + 1)
    all_wait(k_send, k_got, 0)
    unpack(k_got, mid.k)
    mid.diagonal(mid_span, mid_span, None)
    big, small = cells((cx * cy, mx * my), 1), cells((cx * cy, mx * my), 0)
    join = ones_where((big // my // 2 == small // cy) & (big % my // 2 == small % cy))
    join_z = ones_where(cells((mz, cz), 0) // 2 == cells((mz, cz), 1))

    def to_low(values):
        flat = pick(join, pick(values.reshape(mx * my, mz), join_z)) * 0.125
        return flat.reshape(cx, cy, cz)

    low.k[1 : cx + 1] = to_low(mid.k[1 : mx + 1])
    low.diagonal(low_span, low_span, None)

    all_wait(b_send, b_got, 1)
    unpack(b_got, b_mid)
    mid.r[1 : mx + 1] = b_mid[1 : mx + 1]
    mid.first_update(mid_span, centre)
    x_mid[...] = mid.d[1 : mx + 1]
    for number in range(DEGREE):
        pair = weights[number] if number < DEGREE - 1 else None
        mid.apply(mid_span, mid_span, pair)
        if pair is not None:
            x_mid[...] += mid.d[1 : mx + 1]

    near_wait(r_send, far, 2)
    z_start(far, 2)

    low.r[1 : cx + 1] = to_low(mid.r[1 : mx + 1])
    low_centre, low_weights = chebyshev_coefs(COARSE_DEGREE, coarse_low)
    low.first_update(low_span, low_centre)
    x_low[...] = low.d[1 : cx + 1]
    for pair in low_weights:
        low.apply(low_span, low_span, pair)
        x_low[...] += low.d[1 : cx + 1]

    spread = ones_where(
        (cells((mx * my, cx * cy), 0) // my // 2 == cells((mx * my, cx * cy), 1) // cy)
        & (cells((mx * my, cx * cy), 0) % my // 2 == cells((mx * my, cx * cy), 1) % cy)
    )
    spread_z = ones_where(cells((cz, mz), 0) == cells((cz, mz), 1) // 2)
    fixed = pick(spread, pick(x_low[...].reshape(cx * cy, cz), spread_z))
    mid.d[1 : mx + 1] = x_mid[...] + fixed.reshape(mx, my, mz)
    mid.r[1 : mx + 1] = b_mid[1 : mx + 1]
    x_mid[...] = mid.d[1 : mx + 1]
    mid.apply(mid_span, mid_span, (0.0, 1.0 / centre))
    x_mid[...] += mid.d[1 : mx + 1]
    for pair in weights:
        mid.apply(mid_span, mid_span, pair)
        x_mid[...] += mid.d[1 : mx + 1]

    z_finish(far, 2)
    wide = bx + bx // 2
    shape = (wide * 3 * by, mx * my)
    fine_row, mid_row = cells(shape, 0) % (3 * by), cells(shape, 1)
    fine_y = iy * by + jnp.where(fine_row < 2 * by, fine_row, fine_row - 3 * by)
    mid_x = ix * (bx // 2) + cells(shape, 0) // (3 * by) - bx // 2
    rows = ones_where((mid_row // my == mid_x) & (2 * (mid_row % my) == fine_y - fine_y % 2))
    shape = (mz, bz + 128)
    fine_col = cells(shape, 1)
    fine_z = iz * bz + jnp.where(fine_col < bz + 64, fine_col, fine_col - (bz + 128))
    columns = ones_where((fine_z >= 2 * cells(shape, 0)) & (fine_z <= 2 * cells(shape, 0) + 1))
    fixed = pick(rows, pick(x_mid[...].reshape(mx * my, mz), columns))
    fixed = fixed.reshape(wide, 3 * by, bz + 128)
    for p in range(bx - reach, 2 * bx + reach):
        fine.d[p] = fixed[p // 2]
    x_out[...] += fine.d[own]

    def restore(p, carry):
        fine.r[p] = far[p]
        return carry

    lax.fori_loop(*span(4), restore, 0)
    fine.apply(span(5), span(4), (0.0, 1.0 / centre))
    x_out[...] += fine.d[own]
    for number in range(DEGREE):
        pair = weights[number] if number < DEGREE - 1 else None
        fine.apply(span(4 - number), span(3 - number), pair)
        if pair is not None:
            x_out[...] += fine.d[own]
    r_out[...] = fine.r[own]


def gathered(sizes, conductivity, source):
    (nx, ny, nz) = sizes
    (bx, by, bz) = conductivity.shape
    count = nx * ny * nz
    mid = (nx * bx // 2 + 2, ny * by // 2, nz * bz // 2)
    low = (nx * bx // 4 + 2, ny * by // 4, nz * bz // 4)
    window = (3 * bx, 3 * by, bz + 128)
    kept = lambda shape: pltpu.VMEM(shape, jnp.float32)
    inner_mid = (mid[0] - 2, *mid[1:])
    sent = (bx * by // 32, 8, bz // 2)
    groups = (bx + 10 + 15) // 16
    scratch = [kept(window)] * 8 + [kept(mid)] * 8 + [kept(low)] * 8
    scratch += [kept(window), kept(inner_mid), kept(mid), kept((low[0] - 2, *low[1:]))]
    scratch += [kept(sent), kept(sent), kept((bx, by, bz))]
    scratch += [kept((count, *sent)), kept((count, *sent))]
    scratch += [kept((3, 2, groups, 3 * by, 128)), kept((3, 2, groups, 3 * by, 128))]
    dma = pltpu.SemaphoreType.DMA
    scratch += [dma((3, 9)), dma((3, 9)), dma((3, 2)), dma((3, 2)), dma((2, count)), dma((2, count))]
    shape = jax.ShapeDtypeStruct((bx, by, bz), jnp.float32)
    vmem = pl.BlockSpec(memory_space=pltpu.VMEM)
    return pl.pallas_call(
        functools.partial(kernel, sizes, (bx, by, bz)),
        out_shape=(shape, shape),
        in_specs=[vmem, vmem],
        out_specs=(vmem, vmem),
        scratch_shapes=scratch,
        compiler_params=pltpu.CompilerParams(
            collective_id=0, has_side_effects=True, vmem_limit_bytes=48 * 1024 * 1024
        ),
    )(conductivity, source)


def plan(conductivity, source):
    sizes = tuple(lax.axis_size(axis) for axis in ("gx", "gy", "gz"))
    (bx, by, bz) = conductivity.shape
    count = sizes[0] * sizes[1] * sizes[2]
    fits = bx == 8 and by == 8 and bz % 256 == 0 and sizes[1] % 2 == 0
    if fits and count > 1 and count * bx * by * bz // 8 * 4 * 16 <= 16 * 1024 * 1024:
        return gathered(sizes, conductivity, source)
    return body(conductivity, source)


def solution(mesh):
    in_specs = (P("gx", "gy", "gz"), P("gx", "gy", "gz"))
    out_specs = (P("gx", "gy", "gz"), P("gx", "gy", "gz"))
    return jax.shard_map(plan, mesh=mesh, in_specs=in_specs, out_specs=out_specs, check_vma=False)
```

```python
import functools

import jax
import jax.numpy as jnp
from jax import lax
from jax.experimental import pallas as pl
from jax.experimental.pallas import tpu as pltpu
from jax.sharding import PartitionSpec as P

LEVELS = 3
DEGREE = 4
COARSE_DEGREE = 8
MESH = pl.DeviceIdType.MESH


weight_table = {1: 14.0 / 30.0, 2: 3.0 / 30.0, 3: 1.0 / 30.0}
neighbour_offsets = [
    (along_one, along_two, along_three)
    for along_one in (-1, 0, 1)
    for along_two in (-1, 0, 1)
    for along_three in (-1, 0, 1)
    if (along_one, along_two, along_three) != (0, 0, 0)
]
smooth_low = 0.5
coarse_low = 0.03
upper_bound = 2.0


def padded_2(block, sides, width):
    for axis, dim in sides:
        count = lax.axis_size(axis)
        forward = [(i, i + 1) for i in range(count - 1)]
        backward = [(target, source) for source, target in forward]
        low = lax.ppermute(
            lax.slice_in_dim(block, block.shape[dim] - width, None, axis=dim), axis, forward
        )
        high = lax.ppermute(lax.slice_in_dim(block, 0, width, axis=dim), axis, backward)
        block = jnp.concatenate([low, block, high], axis=dim)
    return block


def shifted(padded, offset):
    return padded[
        1 + offset[0] : padded.shape[0] - 1 + offset[0],
        1 + offset[1] : padded.shape[1] - 1 + offset[1],
        1 + offset[2] : padded.shape[2] - 1 + offset[2],
    ]


def inner(values, margin):
    return values[
        margin : values.shape[0] - margin,
        margin : values.shape[1] - margin,
        margin : values.shape[2] - margin,
    ]


def stencil(field_pad, coeff_pad, spacing):
    centre_field = shifted(field_pad, (0, 0, 0))
    centre_coeff = shifted(coeff_pad, (0, 0, 0))
    total = jnp.zeros(centre_field.shape, jnp.float32)
    for offset in neighbour_offsets:
        weight = weight_table[abs(offset[0]) + abs(offset[1]) + abs(offset[2])]
        total = total + weight * (centre_coeff + shifted(coeff_pad, offset)) * (
            centre_field - shifted(field_pad, offset)
        )
    return total * (0.5 / spacing)


def diagonal_of(coeff_pad, spacing):
    centre_coeff = shifted(coeff_pad, (0, 0, 0))
    total = jnp.zeros(centre_coeff.shape, jnp.float32)
    for offset in neighbour_offsets:
        weight = weight_table[abs(offset[0]) + abs(offset[1]) + abs(offset[2])]
        total = total + weight * (centre_coeff + shifted(coeff_pad, offset))
    return total * (0.5 / spacing)


def coarsen(values):
    extent = values.shape
    return values.reshape(extent[0] // 2, 2, extent[1] // 2, 2, extent[2] // 2, 2).mean(
        axis=(1, 3, 5)
    )


def refine(values):
    return jnp.repeat(jnp.repeat(jnp.repeat(values, 2, axis=0), 2, axis=1), 2, axis=2)


def chebyshev_coefs(degree, lower):
    centre = (upper_bound + lower) / 2.0
    half_width = (upper_bound - lower) / 2.0
    ratio_term = centre / half_width
    rho_prev = 1.0 / ratio_term
    weights = []
    for number in range(1, degree):
        rho_next = 1.0 / (2.0 * ratio_term - rho_prev)
        weights.append((rho_next * rho_prev, 2.0 * rho_next / half_width))
        rho_prev = rho_next
    return (centre, weights)


def inside_mask(extent, margin):
    first_pos = (
        lax.axis_index("gx") * extent[0]
        + jnp.arange(extent[0] + 2 * margin, dtype=jnp.int32)
        - margin
    )
    second_pos = (
        lax.axis_index("gy") * extent[1]
        + jnp.arange(extent[1] + 2 * margin, dtype=jnp.int32)
        - margin
    )
    third_pos = (
        lax.axis_index("gz") * extent[2]
        + jnp.arange(extent[2] + 2 * margin, dtype=jnp.int32)
        - margin
    )
    first_ok = (first_pos >= 0) & (first_pos < extent[0] * lax.axis_size("gx"))
    second_ok = (second_pos >= 0) & (second_pos < extent[1] * lax.axis_size("gy"))
    third_ok = (third_pos >= 0) & (third_pos < extent[2] * lax.axis_size("gz"))
    return first_ok[:, None, None] & second_ok[None, :, None] & third_ok[None, None, :]


def operate_near(context, field):
    spacing, coeff_ext, diagonal_ext, inside = context
    padded = padded_2(field, (("gx", 0), ("gy", 1), ("gz", 2)), 1)
    return stencil(padded, inner(coeff_ext, 1), spacing)


def two_steps(context, solution, residual, update, first_pair, second_pair):
    spacing, coeff_ext, diagonal_ext, inside = context
    diagonal = inner(diagonal_ext, 1)
    stacked = jnp.stack([update, residual])
    padded = padded_2(stacked, (("gx", 1), ("gy", 2), ("gz", 3)), 2)
    update_wide = padded[0]
    residual_wide = padded[1]
    residual_near = inner(residual_wide, 1) - stencil(update_wide, coeff_ext, spacing)
    update_near = (
        first_pair[0] * inner(update_wide, 1) + first_pair[1] * residual_near / diagonal_ext
    )
    update_near = jnp.where(inside, update_near, 0.0)
    solution = solution + inner(update_near, 1)
    residual = inner(residual_near, 1) - stencil(update_near, inner(coeff_ext, 1), spacing)
    if second_pair is None:
        update = inner(update_near, 1)
    else:
        update = second_pair[0] * inner(update_near, 1) + second_pair[1] * residual / diagonal
        solution = solution + update
    return (solution, residual, update)


def relax(context, right_side, start, degree, lower, final):
    diagonal = inner(context[2], 1)
    centre, weights = chebyshev_coefs(degree, lower)
    if start is None:
        residual = right_side
    else:
        residual = right_side - operate_near(context, start)
    update = residual / (centre * diagonal)
    solution = update if start is None else start + update
    plan_list = list(weights) + ([None] if final else [])
    position = 0
    while position + 1 < len(plan_list):
        solution, residual, update = two_steps(
            context, solution, residual, update, plan_list[position], plan_list[position + 1]
        )
        position = position + 2
    leftover = plan_list[position:]
    for pair in leftover:
        residual = residual - operate_near(context, update)
        update = pair[0] * update + pair[1] * residual / diagonal
        solution = solution + update
    return (solution, residual)


def body(conductivity, source):
    coeff_now = conductivity
    contexts = []
    for grid_level in range(LEVELS):
        if grid_level > 0:
            coeff_now = coarsen(coeff_now)
        spacing = float(4**grid_level)
        coeff_ext = padded_2(coeff_now, (("gx", 0), ("gy", 1), ("gz", 2)), 2)
        inside = inside_mask(coeff_now.shape, 1)
        diagonal_ext = jnp.where(inside, diagonal_of(coeff_ext, spacing), 1.0)
        contexts.append((spacing, coeff_ext, diagonal_ext, inside))

    def cycle(grid_level, right_side):
        context = contexts[grid_level]
        if grid_level == LEVELS - 1:
            return relax(context, right_side, None, COARSE_DEGREE, coarse_low, False)
        solution, residual = relax(context, right_side, None, DEGREE, smooth_low, True)
        correction, ignored = cycle(grid_level + 1, coarsen(residual))
        solution = solution + refine(correction)
        return relax(context, right_side, solution, DEGREE, smooth_low, grid_level == 0)

    return cycle(0, source)


def part_of(values, size):
    if size & (size - 1) == 0:
        return values >> (size.bit_length() - 1)
    return values // size


def rest_of(values, size):
    if size & (size - 1) == 0:
        return values & (size - 1)
    return values % size


def fold(values, eighth):
    side = jnp.where(eighth, values[8:16], values[16:24])
    return jnp.concatenate([values[0:8], side], axis=0)


def over(span, step):
    if isinstance(span[0], int):
        planes = span[1] - span[0]
        if planes <= 4:
            for p in range(*span):
                step(p)
            return
        size = 2 if planes % 2 == 0 else 1
        trips = planes // size
    else:
        size = 2
        trips = (span[1] - span[0] + 1) >> 1

    def body_of(i, carry):
        for j in range(size):
            step(span[0] + size * i + j)
        return carry

    lax.fori_loop(0, trips, body_of, 0)


def cells(shape, dim):
    return lax.broadcasted_iota(jnp.int32, shape, dim)


def pick(left, right):
    if left.dtype == jnp.bfloat16:
        dense, other, swap = right, left, False
    else:
        dense, other, swap = left, right, True
    total = None
    for _ in range(3):
        part = dense.astype(jnp.bfloat16)
        dense = dense - part.astype(jnp.float32)
        pair = (part, other) if swap else (other, part)
        term = jnp.dot(*pair, preferred_element_type=jnp.float32)
        total = term if total is None else total + term
    return total


def ones_where(condition):
    return jnp.where(condition, 1.0, 0.0).astype(jnp.bfloat16)


def turn(values, shift, dim):
    return pltpu.roll(values, shift % values.shape[dim], dim)


def pair_sum(values, dim, edges):
    low = turn(values, 1, dim)
    high = turn(values, -1, dim)
    if edges is not None:
        low = jnp.where(edges[dim][0], 0.0, low)
        high = jnp.where(edges[dim][1], 0.0, high)
    return low + high


def plane_sums(values, edges):
    beside = pair_sum(values, 1, edges)
    strong = 14.0 * values + 3.0 * beside
    weak = 3.0 * values + beside
    return pair_sum(strong, 0, edges) + 14.0 * beside, pair_sum(weak, 0, edges) + strong


class Level:
    def __init__(self, refs, scale, wide_refs=None):
        self.k, self.r, self.d, self.di, self.dg, self.e, self.f, self.g = refs
        self.scale = scale
        shape = self.k.shape[1:]
        self.wide_refs = wide_refs
        self.edges = None
        if wide_refs is None:
            self.edges = [
                (cells(shape, dim) == 0, cells(shape, dim) == shape[dim] - 1) for dim in (0, 1)
            ]
        else:
            self.eighth = cells((8, shape[1]), 0) < 4

    def folded(self, values):
        return values if self.wide_refs is None else fold(values, self.eighth)

    def diagonal(self, wide, near, inside):
        def first(p):
            coeff = self.k[p] if self.wide_refs is None else self.wide_refs[0][p]
            here, side = plane_sums(coeff, self.edges)
            self.e[p] = self.folded(here)
            self.g[p] = self.folded(side)
            if self.wide_refs is not None:
                self.k[p] = self.folded(coeff)

        over(wide, first)

        def second(p):
            total = 128.0 * self.k[p] + self.e[p] + (self.g[p - 1] + self.g[p + 1])
            total = total * self.scale
            self.dg[p] = total
            good = (total > 0.0) & (self.k[p] > 0.0)
            if inside is not None:
                good = good & inside
            self.di[p] = jnp.where(good, 1.0 / total, 0.0)

        over(near, second)

    def first_update(self, span, centre):
        def step(p):
            self.d[p] = self.r[p] * self.di[p] * (1.0 / centre)

        over(span, step)

    def apply(self, wide, near, pair, whole=False):
        def first(p):
            field = self.wide_refs[1][p] if whole else self.d[p]
            coeff = self.wide_refs[0][p] if whole else self.k[p]
            here, side = plane_sums(field, self.edges)
            here_k, side_k = plane_sums(coeff * field, self.edges)
            around = coeff * here + here_k
            if whole:
                around, side, side_k = (self.folded(part) for part in (around, side, side_k))
                self.d[p] = self.folded(field)
            self.e[p] = around
            self.f[p] = side
            self.g[p] = side_k

        over(wide, first)

        def second(p):
            field = self.d[p]
            around = self.e[p] + self.k[p] * (self.f[p - 1] + self.f[p + 1])
            around = around + (self.g[p - 1] + self.g[p + 1])
            left = self.r[p] - (self.dg[p] * field - self.scale * around)
            self.r[p] = left
            if pair is not None:
                fresh = pair[1] * (left * self.di[p])
                self.d[p] = fresh if pair[0] == 0.0 else pair[0] * field + fresh

        over(near, second)


def kernel(sizes, block, *refs):
    (nx, ny, nz) = sizes
    (bx, by, bz) = block
    count = nx * ny * nz
    (k_in, b_in, x_out, r_out) = refs[:4]
    fine_refs = refs[4:12]
    mid_refs = refs[12:20]
    low_refs = refs[20:28]
    (x_mid, b_mid, x_low) = refs[28:31]
    (k_send, b_send, r_send, k_got, b_got) = refs[31:36]
    (k_near, b_near, r_near, d_wide) = refs[36:40]
    packs_out, packs_in = refs[40:43], refs[43:46]
    (halo_out, halo_in, z_out, z_in, all_out, all_in) = refs[46:52]
    (rows_keep, columns_keep) = refs[52:54]
    ix, iy, iz = lax.axis_index("gx"), lax.axis_index("gy"), lax.axis_index("gz")
    me = (ix * ny + iy) * nz + iz
    reach = 5

    def place(number):
        return (number // (ny * nz), (number // nz) % ny, number % nz)

    def clear(ref, planes):
        def step(p):
            ref[p] = jnp.zeros(ref.shape[1:], jnp.float32)

        if isinstance(planes, list):
            for p in planes:
                step(p)
        else:
            over(planes, step)

    for ref in (k_near, b_near, r_near):
        clear(ref, (bx - reach - 1, 2 * bx + reach + 1))

    barrier = pltpu.get_barrier_semaphore()

    def greet(j, carry):
        pl.semaphore_signal(
            barrier, inc=1, device_id=place((me + j) % count), device_id_type=MESH
        )
        return carry

    lax.fori_loop(1, count, greet, 0)
    pl.semaphore_wait(barrier, count - 1)

    fine = Level(fine_refs, 0.5 / 30.0, (k_near, d_wide))
    mid = Level(mid_refs, 0.5 / 4.0 / 30.0)
    low = Level(low_refs, 0.5 / 16.0 / 30.0)

    def near_copy(source, target, which, dx, dy):
        deep = reach if which == 0 else reach - 1
        planes = bx if dx == 0 else deep
        first_from = 0 if dx <= 0 else bx - deep
        first_to = {0: bx, 1: bx - deep, -1: 2 * bx}[dx]
        row_to = {0: 0, 1: 2 * by, -1: by}[dy]
        number = (dx + 1) * 3 + dy + 1
        return pltpu.make_async_remote_copy(
            src_ref=source.at[pl.ds(first_from, planes)],
            dst_ref=target.at[pl.ds(first_to, planes), pl.ds(row_to, by), pl.ds(0, bz)],
            send_sem=halo_out.at[which, number],
            recv_sem=halo_in.at[which, number],
            device_id=(ix + dx, iy + dy, iz),
            device_id_type=MESH,
        )

    sides = [(dx, dy) for dx in (0, 1, -1) for dy in (1, -1, 0) if (dx, dy) != (0, 0)]

    def present(dx, dy):
        return (ix + dx >= 0) & (ix + dx < nx) & (iy + dy >= 0) & (iy + dy < ny)

    def near_start(source, target, which):
        for dx, dy in sides:
            @pl.when(present(dx, dy))
            def _():
                near_copy(source, target, which, dx, dy).start()

    def near_wait(source, target, which):
        for dx, dy in sides:
            @pl.when(present(-dx, -dy))
            def _():
                near_copy(source, target, which, dx, dy).wait_recv()

            @pl.when(present(dx, dy))
            def _():
                near_copy(source, target, which, dx, dy).wait_send()

    eighth = cells((8, bz), 0) < 4

    def z_planes(which):
        deep = reach if which == 0 else reach - 1
        planes = list(range(bx - deep, 2 * bx + deep))
        return [planes[i : i + 16] for i in range(0, len(planes), 16)]

    def z_copy(which, side):
        return pltpu.make_async_remote_copy(
            src_ref=packs_out[which].at[side],
            dst_ref=packs_in[which].at[side],
            send_sem=z_out.at[which, side],
            recv_sem=z_in.at[which, side],
            device_id=(ix, iy, iz + (1 if side == 0 else -1)),
            device_id_type=MESH,
        )

    to_there = (iz + 1 < nz, iz > 0)
    from_there = (iz > 0, iz + 1 < nz)

    def z_start(window, which):
        pack = packs_out[which]
        lane = cells(pack.shape[2:], 1)
        for group, planes in enumerate(z_planes(which)):
            up = jnp.zeros(pack.shape[2:], jnp.float32)
            down = jnp.zeros(pack.shape[2:], jnp.float32)
            for i, p in enumerate(planes):
                mine = (lane >> 3) == i
                up = jnp.where(mine, turn(window[p, :, bz - 128 : bz], 8 * i + 8, 1), up)
                down = jnp.where(mine, turn(window[p, :, 0:128], 8 * i, 1), down)
            pack[0, group] = up
            pack[1, group] = down
        for side in (0, 1):
            @pl.when(to_there[side])
            def _():
                z_copy(which, side).start()

    def z_finish(window, which):
        pack = packs_in[which]
        lane = cells(pack.shape[2:], 1)
        for side in (0, 1):
            @pl.when(from_there[side])
            def _():
                z_copy(which, side).wait_recv()

            @pl.when(jnp.logical_not(from_there[side]))
            def _():
                pack[side] = jnp.zeros(pack.shape[1:], jnp.float32)

            @pl.when(to_there[side])
            def _():
                z_copy(which, side).wait_send()

        for group, planes in enumerate(z_planes(which)):
            below = pack[0, group]
            above = pack[1, group]
            for i, p in enumerate(planes):
                window[p, :, bz : bz + 128] = jnp.where(
                    lane < 64, turn(above, -8 * i, 1), turn(below, -8 * i - 8, 1)
                )

    def fold_in(window):
        for p in z_planes(1)[0]:
            fine.r[p, :, 0:bz] = fold(window[p, :, 0:bz], eighth)

    def all_copy(source, target, which, peer, slot):
        return pltpu.make_async_remote_copy(
            src_ref=source,
            dst_ref=target.at[slot],
            send_sem=all_out.at[which, peer],
            recv_sem=all_in.at[which, slot],
            device_id=place(peer),
            device_id_type=MESH,
        )

    def all_start(source, target, which):
        target[me] = source[...]

        def step(j, carry):
            all_copy(source, target, which, (me + j) % count, me).start()
            return carry

        lax.fori_loop(1, count, step, 0)

    def all_wait(source, target, which):
        def step(j, carry):
            peer = (me + j) % count
            all_copy(source, target, which, peer, peer).wait_recv()
            all_copy(source, target, which, peer, me).wait_send()
            return carry

        lax.fori_loop(1, count, step, 0)

    half = bx // 2 * (by // 2)
    to_row, from_row = cells((half, bx * by), 0), cells((half, bx * by), 1)
    shrink = ones_where(
        (part_of(from_row, 2 * by) == part_of(to_row, by // 2))
        & (rest_of(from_row, by) >> 1 == rest_of(to_row, by // 2))
    )
    shrink_z = ones_where(cells((bz, bz // 2), 0) >> 1 == cells((bz, bz // 2), 1))

    def coarse_block(values):
        flat = pick(pick(shrink, values.reshape(bx * by, bz)), shrink_z) * 0.125
        return flat.reshape(half // 8, 8, bz // 2)

    row8 = cells((8, bz // 2), 0)

    def unpack(got, target):
        for jx in range(nx):
            for jy in range(0, ny, 2):
                for jz in range(nz):
                    slot = (jx * ny + jy) * nz + jz
                    for t in range(half // 8):
                        one, two = got[slot, t], got[slot + nz, t]
                        p = 1 + jx * (bx // 2) + 2 * t
                        at = (slice(jy * 4, jy * 4 + 8), slice(jz * bz // 2, (jz + 1) * bz // 2))
                        target[(p, *at)] = jnp.where(row8 < 4, one, turn(two, 4, 0))
                        target[(p + 1, *at)] = jnp.where(row8 < 4, turn(one, 4, 0), two)

    near_start(k_in, k_near, 0)
    near_start(b_in, b_near, 1)
    k_send[...] = coarse_block(k_in[...])
    k_near[bx : 2 * bx, 0:by, 0:bz] = k_in[...]
    b_near[bx : 2 * bx, 0:by, 0:bz] = b_in[...]
    edge = bx - reach - 1
    for ref in fine_refs:
        clear(ref, [edge, bx - 1, 2 * bx, 2 * bx + 1, 2 * bx + reach])
        clear(ref, (edge, bx))
        clear(ref, (2 * bx, 2 * bx + reach + 1))
    clear(d_wide, [2 * bx + reach])
    for ref in (mid.f, mid.g):
        clear(ref, [0, ref.shape[0] - 1])
    for ref in (low.f, low.g):
        clear(ref, [0, ref.shape[0] - 1])
    mx, my, mz = mid.k.shape[0] - 2, mid.k.shape[1], mid.k.shape[2]
    wide = bx + bx // 2
    mid_x = ix * (bx // 2) - bx // 2
    for q in range(wide):
        shape = (3 * by, mx * my)
        fine_row, mid_row = cells(shape, 0), cells(shape, 1)
        fine_y = iy * by + jnp.where(fine_row < 2 * by, fine_row, fine_row - 3 * by)
        target = (mid_x + q) * my + (fine_y >> 1)
        good = (fine_y >= 0) & (fine_y < ny * by) & (mid_x + q >= 0) & (mid_x + q < mx)
        rows_keep[q] = jnp.where((mid_row == target) & good, 1.0, 0.0)
    shape = (mz, bz + 128)
    fine_col = cells(shape, 1)
    fine_z = iz * bz + jnp.where(fine_col < bz + 64, fine_col, fine_col - (bz + 128))
    columns_keep[...] = ones_where((fine_z >> 1) == cells(shape, 0))
    near_wait(k_in, k_near, 0)
    z_start(k_near, 0)
    near_wait(b_in, b_near, 1)
    fold_in(b_near)
    z_start(fine.r, 1)
    all_start(k_send, k_got, 0)
    z_finish(k_near, 0)

    def span(width):
        return (
            jnp.maximum(bx - width, bx - ix * bx),
            jnp.minimum(2 * bx + width, bx + (nx - ix) * bx),
        )

    plane = (2 * by, bz + 128)
    row, col = cells(plane, 0), cells(plane, 1)
    inside = (
        (row < by) | ((row < by + 4) & (iy + 1 < ny)) | ((row >= by + 4) & (iy > 0))
    ) & ((col < bz) | ((col < bz + 64) & (iz + 1 < nz)) | ((col >= bz + 64) & (iz > 0)))
    fine.diagonal(span(5), span(4), inside)
    z_finish(fine.r, 1)

    own = (slice(bx, 2 * bx), slice(0, by), slice(0, bz))
    centre, weights = chebyshev_coefs(DEGREE, smooth_low)
    fine.first_update(span(4), centre)
    x_out[...] = fine.d[own]
    for number in range(DEGREE):
        pair = weights[number] if number < DEGREE - 1 else None
        fine.apply(span(4 - number), span(3 - number), pair)
        if pair is not None:
            x_out[...] += fine.d[own]

    r_send[...] = fine.r[own]
    b_send[...] = coarse_block(r_send[...])
    all_start(b_send, b_got, 1)
    near_start(r_send, r_near, 2)
    r_near[own] = r_send[...]

    cx, cy, cz = mx // 2, my // 2, mz // 2
    mid_span, low_span = (1, mx + 1), (1, cx + 1)
    all_wait(k_send, k_got, 0)
    unpack(k_got, mid.k)
    mid.diagonal(mid_span, mid_span, None)
    big, small = cells((cx * cy, mx * my), 1), cells((cx * cy, mx * my), 0)
    join = ones_where(
        (part_of(big, 2 * my) == part_of(small, cy)) & (rest_of(big, my) >> 1 == rest_of(small, cy))
    )
    join_z = ones_where(cells((mz, cz), 0) >> 1 == cells((mz, cz), 1))

    def to_low(values):
        flat = pick(join, pick(values.reshape(mx * my, mz), join_z)) * 0.125
        return flat.reshape(cx, cy, cz)

    low.k[1 : cx + 1] = to_low(mid.k[1 : mx + 1])
    low.diagonal(low_span, low_span, None)

    all_wait(b_send, b_got, 1)
    unpack(b_got, b_mid)
    mid.r[1 : mx + 1] = b_mid[1 : mx + 1]
    mid.first_update(mid_span, centre)
    x_mid[...] = mid.d[1 : mx + 1]
    for number in range(DEGREE):
        pair = weights[number] if number < DEGREE - 1 else None
        mid.apply(mid_span, mid_span, pair)
        if pair is not None:
            x_mid[...] += mid.d[1 : mx + 1]

    near_wait(r_send, r_near, 2)
    fold_in(r_near)
    z_start(fine.r, 2)

    low.r[1 : cx + 1] = to_low(mid.r[1 : mx + 1])
    low_centre, low_weights = chebyshev_coefs(COARSE_DEGREE, coarse_low)
    low.first_update(low_span, low_centre)
    x_low[...] = low.d[1 : cx + 1]
    for pair in low_weights:
        low.apply(low_span, low_span, pair)
        x_low[...] += low.d[1 : cx + 1]

    big, small = cells((mx * my, cx * cy), 0), cells((mx * my, cx * cy), 1)
    spread = ones_where(
        (part_of(big, 2 * my) == part_of(small, cy)) & (rest_of(big, my) >> 1 == rest_of(small, cy))
    )
    spread_z = ones_where(cells((cz, mz), 0) == cells((cz, mz), 1) >> 1)
    fixed = pick(spread, pick(x_low[...].reshape(cx * cy, cz), spread_z))
    mid.d[1 : mx + 1] = x_mid[...] + fixed.reshape(mx, my, mz)
    mid.r[1 : mx + 1] = b_mid[1 : mx + 1]
    x_mid[...] = mid.d[1 : mx + 1]
    mid.apply(mid_span, mid_span, (0.0, 1.0 / centre))
    x_mid[...] += mid.d[1 : mx + 1]
    for pair in weights:
        mid.apply(mid_span, mid_span, pair)
        x_mid[...] += mid.d[1 : mx + 1]

    z_finish(fine.r, 2)
    rows = rows_keep[...].reshape(wide * 3 * by, mx * my).astype(jnp.bfloat16)
    fixed = pick(rows, pick(x_mid[...].reshape(mx * my, mz), columns_keep[...]))
    fixed = fixed.reshape(wide, 3 * by, bz + 128)
    for p in range(bx - reach, 2 * bx + reach):
        d_wide[p] = fixed[p // 2]
    x_out[...] += d_wide[own]
    fine.apply(span(5), span(4), (0.0, 1.0 / centre), True)
    x_out[...] += fine.d[own]
    for number in range(DEGREE):
        pair = weights[number] if number < DEGREE - 1 else None
        fine.apply(span(4 - number), span(3 - number), pair)
        if pair is not None:
            x_out[...] += fine.d[own]
    r_out[...] = fine.r[own]


def gathered(sizes, conductivity, source):
    (nx, ny, nz) = sizes
    (bx, by, bz) = conductivity.shape
    count = nx * ny * nz
    mid = (nx * bx // 2 + 2, ny * by // 2, nz * bz // 2)
    low = (nx * bx // 4 + 2, ny * by // 4, nz * bz // 4)
    window = (3 * bx, 3 * by, bz + 128)
    narrow = (3 * bx, 2 * by, bz + 128)
    kept = lambda shape: pltpu.VMEM(shape, jnp.float32)
    inner_mid = (mid[0] - 2, *mid[1:])
    sent = (bx * by // 32, 8, bz // 2)
    scratch = [kept(narrow)] * 8 + [kept(mid)] * 8 + [kept(low)] * 8
    scratch += [kept(inner_mid), kept(mid), kept((low[0] - 2, *low[1:]))]
    scratch += [kept(sent), kept(sent), kept((bx, by, bz))]
    scratch += [kept((count, *sent)), kept((count, *sent))]
    scratch += [kept(window)] * 4
    packs = [kept((2, 2, 3 * by, 128)), kept((2, 1, 2 * by, 128)), kept((2, 1, 2 * by, 128))]
    scratch += packs + packs
    dma = pltpu.SemaphoreType.DMA
    scratch += [dma((3, 9)), dma((3, 9)), dma((3, 2)), dma((3, 2)), dma((2, count)), dma((2, count))]
    scratch += [kept((bx + bx // 2, 3 * by, inner_mid[0] * inner_mid[1]))]
    scratch += [pltpu.VMEM((inner_mid[2], bz + 128), jnp.bfloat16)]
    shape = jax.ShapeDtypeStruct((bx, by, bz), jnp.float32)
    vmem = pl.BlockSpec(memory_space=pltpu.VMEM)
    return pl.pallas_call(
        functools.partial(kernel, sizes, (bx, by, bz)),
        out_shape=(shape, shape),
        in_specs=[vmem, vmem],
        out_specs=(vmem, vmem),
        scratch_shapes=scratch,
        compiler_params=pltpu.CompilerParams(
            collective_id=0, has_side_effects=True, vmem_limit_bytes=48 * 1024 * 1024
        ),
    )(conductivity, source)


def plan(conductivity, source):
    sizes = tuple(lax.axis_size(axis) for axis in ("gx", "gy", "gz"))
    (bx, by, bz) = conductivity.shape
    count = sizes[0] * sizes[1] * sizes[2]
    fits = bx == 8 and by == 8 and bz % 256 == 0 and sizes[1] % 2 == 0
    if fits and count > 1 and count * bx * by * bz // 8 * 4 * 16 <= 16 * 1024 * 1024:
        return gathered(sizes, conductivity, source)
    return body(conductivity, source)


def solution(mesh):
    in_specs = (P("gx", "gy", "gz"), P("gx", "gy", "gz"))
    out_specs = (P("gx", "gy", "gz"), P("gx", "gy", "gz"))
    return jax.shard_map(plan, mesh=mesh, in_specs=in_specs, out_specs=out_specs, check_vma=False)
```

```python
import functools

import jax
import jax.numpy as jnp
from jax import lax
from jax.experimental import pallas as pl
from jax.experimental.pallas import tpu as pltpu
from jax.sharding import PartitionSpec as P

LEVELS = 3
DEGREE = 4
COARSE_DEGREE = 8
MESH = pl.DeviceIdType.MESH


weight_table = {1: 14.0 / 30.0, 2: 3.0 / 30.0, 3: 1.0 / 30.0}
neighbour_offsets = [
    (along_one, along_two, along_three)
    for along_one in (-1, 0, 1)
    for along_two in (-1, 0, 1)
    for along_three in (-1, 0, 1)
    if (along_one, along_two, along_three) != (0, 0, 0)
]
smooth_low = 0.5
coarse_low = 0.03
upper_bound = 2.0


def padded_2(block, sides, width):
    for axis, dim in sides:
        count = lax.axis_size(axis)
        forward = [(i, i + 1) for i in range(count - 1)]
        backward = [(target, source) for source, target in forward]
        low = lax.ppermute(
            lax.slice_in_dim(block, block.shape[dim] - width, None, axis=dim), axis, forward
        )
        high = lax.ppermute(lax.slice_in_dim(block, 0, width, axis=dim), axis, backward)
        block = jnp.concatenate([low, block, high], axis=dim)
    return block


def shifted(padded, offset):
    return padded[
        1 + offset[0] : padded.shape[0] - 1 + offset[0],
        1 + offset[1] : padded.shape[1] - 1 + offset[1],
        1 + offset[2] : padded.shape[2] - 1 + offset[2],
    ]


def inner(values, margin):
    return values[
        margin : values.shape[0] - margin,
        margin : values.shape[1] - margin,
        margin : values.shape[2] - margin,
    ]


def stencil(field_pad, coeff_pad, spacing):
    centre_field = shifted(field_pad, (0, 0, 0))
    centre_coeff = shifted(coeff_pad, (0, 0, 0))
    total = jnp.zeros(centre_field.shape, jnp.float32)
    for offset in neighbour_offsets:
        weight = weight_table[abs(offset[0]) + abs(offset[1]) + abs(offset[2])]
        total = total + weight * (centre_coeff + shifted(coeff_pad, offset)) * (
            centre_field - shifted(field_pad, offset)
        )
    return total * (0.5 / spacing)


def diagonal_of(coeff_pad, spacing):
    centre_coeff = shifted(coeff_pad, (0, 0, 0))
    total = jnp.zeros(centre_coeff.shape, jnp.float32)
    for offset in neighbour_offsets:
        weight = weight_table[abs(offset[0]) + abs(offset[1]) + abs(offset[2])]
        total = total + weight * (centre_coeff + shifted(coeff_pad, offset))
    return total * (0.5 / spacing)


def coarsen(values):
    extent = values.shape
    return values.reshape(extent[0] // 2, 2, extent[1] // 2, 2, extent[2] // 2, 2).mean(
        axis=(1, 3, 5)
    )


def refine(values):
    return jnp.repeat(jnp.repeat(jnp.repeat(values, 2, axis=0), 2, axis=1), 2, axis=2)


def chebyshev_coefs(degree, lower):
    centre = (upper_bound + lower) / 2.0
    half_width = (upper_bound - lower) / 2.0
    ratio_term = centre / half_width
    rho_prev = 1.0 / ratio_term
    weights = []
    for number in range(1, degree):
        rho_next = 1.0 / (2.0 * ratio_term - rho_prev)
        weights.append((rho_next * rho_prev, 2.0 * rho_next / half_width))
        rho_prev = rho_next
    return (centre, weights)


def inside_mask(extent, margin):
    first_pos = (
        lax.axis_index("gx") * extent[0]
        + jnp.arange(extent[0] + 2 * margin, dtype=jnp.int32)
        - margin
    )
    second_pos = (
        lax.axis_index("gy") * extent[1]
        + jnp.arange(extent[1] + 2 * margin, dtype=jnp.int32)
        - margin
    )
    third_pos = (
        lax.axis_index("gz") * extent[2]
        + jnp.arange(extent[2] + 2 * margin, dtype=jnp.int32)
        - margin
    )
    first_ok = (first_pos >= 0) & (first_pos < extent[0] * lax.axis_size("gx"))
    second_ok = (second_pos >= 0) & (second_pos < extent[1] * lax.axis_size("gy"))
    third_ok = (third_pos >= 0) & (third_pos < extent[2] * lax.axis_size("gz"))
    return first_ok[:, None, None] & second_ok[None, :, None] & third_ok[None, None, :]


def operate_near(context, field):
    spacing, coeff_ext, diagonal_ext, inside = context
    padded = padded_2(field, (("gx", 0), ("gy", 1), ("gz", 2)), 1)
    return stencil(padded, inner(coeff_ext, 1), spacing)


def two_steps(context, solution, residual, update, first_pair, second_pair):
    spacing, coeff_ext, diagonal_ext, inside = context
    diagonal = inner(diagonal_ext, 1)
    stacked = jnp.stack([update, residual])
    padded = padded_2(stacked, (("gx", 1), ("gy", 2), ("gz", 3)), 2)
    update_wide = padded[0]
    residual_wide = padded[1]
    residual_near = inner(residual_wide, 1) - stencil(update_wide, coeff_ext, spacing)
    update_near = (
        first_pair[0] * inner(update_wide, 1) + first_pair[1] * residual_near / diagonal_ext
    )
    update_near = jnp.where(inside, update_near, 0.0)
    solution = solution + inner(update_near, 1)
    residual = inner(residual_near, 1) - stencil(update_near, inner(coeff_ext, 1), spacing)
    if second_pair is None:
        update = inner(update_near, 1)
    else:
        update = second_pair[0] * inner(update_near, 1) + second_pair[1] * residual / diagonal
        solution = solution + update
    return (solution, residual, update)


def relax(context, right_side, start, degree, lower, final):
    diagonal = inner(context[2], 1)
    centre, weights = chebyshev_coefs(degree, lower)
    if start is None:
        residual = right_side
    else:
        residual = right_side - operate_near(context, start)
    update = residual / (centre * diagonal)
    solution = update if start is None else start + update
    plan_list = list(weights) + ([None] if final else [])
    position = 0
    while position + 1 < len(plan_list):
        solution, residual, update = two_steps(
            context, solution, residual, update, plan_list[position], plan_list[position + 1]
        )
        position = position + 2
    leftover = plan_list[position:]
    for pair in leftover:
        residual = residual - operate_near(context, update)
        update = pair[0] * update + pair[1] * residual / diagonal
        solution = solution + update
    return (solution, residual)


def body(conductivity, source):
    coeff_now = conductivity
    contexts = []
    for grid_level in range(LEVELS):
        if grid_level > 0:
            coeff_now = coarsen(coeff_now)
        spacing = float(4**grid_level)
        coeff_ext = padded_2(coeff_now, (("gx", 0), ("gy", 1), ("gz", 2)), 2)
        inside = inside_mask(coeff_now.shape, 1)
        diagonal_ext = jnp.where(inside, diagonal_of(coeff_ext, spacing), 1.0)
        contexts.append((spacing, coeff_ext, diagonal_ext, inside))

    def cycle(grid_level, right_side):
        context = contexts[grid_level]
        if grid_level == LEVELS - 1:
            return relax(context, right_side, None, COARSE_DEGREE, coarse_low, False)
        solution, residual = relax(context, right_side, None, DEGREE, smooth_low, True)
        correction, ignored = cycle(grid_level + 1, coarsen(residual))
        solution = solution + refine(correction)
        return relax(context, right_side, solution, DEGREE, smooth_low, grid_level == 0)

    return cycle(0, source)


def part_of(values, size):
    if size & (size - 1) == 0:
        return values >> (size.bit_length() - 1)
    return values // size


def rest_of(values, size):
    if size & (size - 1) == 0:
        return values & (size - 1)
    return values % size


def fold(values, eighth):
    side = jnp.where(eighth, values[8:16], values[16:24])
    return jnp.concatenate([values[0:8], side], axis=0)


def over(span, step):
    if isinstance(span[0], int):
        planes = span[1] - span[0]
        if planes <= 4:
            for p in range(*span):
                step(p)
            return
        size = 4 if planes % 4 == 0 else 2 if planes % 2 == 0 else 1
        trips = planes // size
    else:
        size = 2
        trips = (span[1] - span[0] + 1) >> 1

    def body_of(i, carry):
        for j in range(size):
            step(span[0] + size * i + j)
        return carry

    lax.fori_loop(0, trips, body_of, 0)


def cells(shape, dim):
    return lax.broadcasted_iota(jnp.int32, shape, dim)


def pick(left, right):
    if left.dtype == jnp.bfloat16:
        dense, other, swap = right, left, False
    else:
        dense, other, swap = left, right, True
    total = None
    for _ in range(3):
        part = dense.astype(jnp.bfloat16)
        dense = dense - part.astype(jnp.float32)
        pair = (part, other) if swap else (other, part)
        term = jnp.dot(*pair, preferred_element_type=jnp.float32)
        total = term if total is None else total + term
    return total


def ones_where(condition):
    return jnp.where(condition, 1.0, 0.0).astype(jnp.bfloat16)


def turn(values, shift, dim):
    return pltpu.roll(values, shift % values.shape[dim], dim)


def pair_sum(values, dim, edges):
    low = turn(values, 1, dim)
    high = turn(values, -1, dim)
    if edges is not None:
        low = jnp.where(edges[dim][0], 0.0, low)
        high = jnp.where(edges[dim][1], 0.0, high)
    return low + high


def plane_sums(values, edges):
    beside = pair_sum(values, 1, edges)
    strong = 14.0 * values + 3.0 * beside
    weak = 3.0 * values + beside
    return pair_sum(strong, 0, edges) + 14.0 * beside, pair_sum(weak, 0, edges) + strong


class Level:
    def __init__(self, refs, scale, wide_refs=None):
        self.k, self.r, self.d, self.di, self.dg, self.e, self.f, self.g = refs
        self.scale = scale
        shape = self.k.shape[1:]
        self.wide_refs = wide_refs
        self.edges = None
        if wide_refs is None:
            self.edges = [
                (cells(shape, dim) == 0, cells(shape, dim) == shape[dim] - 1) for dim in (0, 1)
            ]
        else:
            self.eighth = cells((8, shape[1]), 0) < 4

    def folded(self, values):
        return values if self.wide_refs is None else fold(values, self.eighth)

    def diagonal(self, wide, near, inside):
        def first(p):
            coeff = self.k[p] if self.wide_refs is None else self.wide_refs[0][p]
            here, side = plane_sums(coeff, self.edges)
            self.e[p] = self.folded(here)
            self.g[p] = self.folded(side)
            if self.wide_refs is not None:
                self.k[p] = self.folded(coeff)

        over(wide, first)

        def second(p):
            total = 128.0 * self.k[p] + self.e[p] + (self.g[p - 1] + self.g[p + 1])
            total = total * self.scale
            self.dg[p] = total
            good = (total > 0.0) & (self.k[p] > 0.0)
            if inside is not None:
                good = good & inside
            self.di[p] = jnp.where(good, 1.0 / total, 0.0)

        over(near, second)

    def first_update(self, span, centre):
        def step(p):
            self.d[p] = self.r[p] * self.di[p] * (1.0 / centre)

        over(span, step)

    def apply(self, wide, near, pair, whole=False):
        def first(p):
            field = self.wide_refs[1][p] if whole else self.d[p]
            coeff = self.wide_refs[0][p] if whole else self.k[p]
            here, side = plane_sums(field, self.edges)
            here_k, side_k = plane_sums(coeff * field, self.edges)
            around = coeff * here + here_k
            if whole:
                around, side, side_k = (self.folded(part) for part in (around, side, side_k))
                self.d[p] = self.folded(field)
            self.e[p] = around
            self.f[p] = side
            self.g[p] = side_k

        over(wide, first)

        def second(p):
            field = self.d[p]
            around = self.e[p] + self.k[p] * (self.f[p - 1] + self.f[p + 1])
            around = around + (self.g[p - 1] + self.g[p + 1])
            left = self.r[p] - (self.dg[p] * field - self.scale * around)
            self.r[p] = left
            if pair is not None:
                fresh = pair[1] * (left * self.di[p])
                self.d[p] = fresh if pair[0] == 0.0 else pair[0] * field + fresh

        over(near, second)


def kernel(sizes, block, *refs):
    (nx, ny, nz) = sizes
    (bx, by, bz) = block
    count = nx * ny * nz
    (k_in, b_in, x_out, r_out) = refs[:4]
    fine_refs = refs[4:12]
    mid_refs = refs[12:20]
    low_refs = refs[20:28]
    (x_mid, b_mid, x_low) = refs[28:31]
    (k_send, b_send, r_send, k_got, b_got) = refs[31:36]
    (k_near, b_near, r_near, d_wide) = refs[36:40]
    packs_out, packs_in = refs[40:43], refs[43:46]
    (halo_out, halo_in, z_out, z_in, all_out, all_in) = refs[46:52]
    (rows_keep, columns_keep) = refs[52:54]
    ix, iy, iz = lax.axis_index("gx"), lax.axis_index("gy"), lax.axis_index("gz")
    me = (ix * ny + iy) * nz + iz
    reach = 5

    def place(number):
        return (number // (ny * nz), (number // nz) % ny, number % nz)

    def clear(ref, planes):
        def step(p):
            ref[p] = jnp.zeros(ref.shape[1:], jnp.float32)

        if isinstance(planes, list):
            for p in planes:
                step(p)
        else:
            over(planes, step)

    for ref in (k_near, b_near, r_near):
        clear(ref, (bx - reach - 1, 2 * bx + reach + 1))

    barrier = pltpu.get_barrier_semaphore()

    def greet(j, carry):
        pl.semaphore_signal(
            barrier, inc=1, device_id=place((me + j) % count), device_id_type=MESH
        )
        return carry

    lax.fori_loop(1, count, greet, 0)
    pl.semaphore_wait(barrier, count - 1)

    fine = Level(fine_refs, 0.5 / 30.0, (k_near, d_wide))
    mid = Level(mid_refs, 0.5 / 4.0 / 30.0)
    low = Level(low_refs, 0.5 / 16.0 / 30.0)

    def near_copy(source, target, which, dx, dy):
        deep = reach if which == 0 else reach - 1
        planes = bx if dx == 0 else deep
        first_from = 0 if dx <= 0 else bx - deep
        first_to = {0: bx, 1: bx - deep, -1: 2 * bx}[dx]
        row_to = {0: 0, 1: 2 * by, -1: by}[dy]
        number = (dx + 1) * 3 + dy + 1
        return pltpu.make_async_remote_copy(
            src_ref=source.at[pl.ds(first_from, planes)],
            dst_ref=target.at[pl.ds(first_to, planes), pl.ds(row_to, by), pl.ds(0, bz)],
            send_sem=halo_out.at[which, number],
            recv_sem=halo_in.at[which, number],
            device_id=(ix + dx, iy + dy, iz),
            device_id_type=MESH,
        )

    sides = [(dx, dy) for dx in (0, 1, -1) for dy in (1, -1, 0) if (dx, dy) != (0, 0)]

    def present(dx, dy):
        return (ix + dx >= 0) & (ix + dx < nx) & (iy + dy >= 0) & (iy + dy < ny)

    def near_start(source, target, which):
        for dx, dy in sides:
            @pl.when(present(dx, dy))
            def _():
                near_copy(source, target, which, dx, dy).start()

    def near_wait(source, target, which):
        for dx, dy in sides:
            @pl.when(present(-dx, -dy))
            def _():
                near_copy(source, target, which, dx, dy).wait_recv()

            @pl.when(present(dx, dy))
            def _():
                near_copy(source, target, which, dx, dy).wait_send()

    eighth = cells((8, bz), 0) < 4

    def z_planes(which):
        deep = reach if which == 0 else reach - 1
        planes = list(range(bx - deep, 2 * bx + deep))
        return [planes[i : i + 16] for i in range(0, len(planes), 16)]

    def z_copy(which, side):
        return pltpu.make_async_remote_copy(
            src_ref=packs_out[which].at[side],
            dst_ref=packs_in[which].at[side],
            send_sem=z_out.at[which, side],
            recv_sem=z_in.at[which, side],
            device_id=(ix, iy, iz + (1 if side == 0 else -1)),
            device_id_type=MESH,
        )

    to_there = (iz + 1 < nz, iz > 0)
    from_there = (iz > 0, iz + 1 < nz)

    def z_start(window, which):
        pack = packs_out[which]
        lane = cells(pack.shape[2:], 1)
        for group, planes in enumerate(z_planes(which)):
            up = jnp.zeros(pack.shape[2:], jnp.float32)
            down = jnp.zeros(pack.shape[2:], jnp.float32)
            for i, p in enumerate(planes):
                mine = (lane >> 3) == i
                up = jnp.where(mine, turn(window[p, :, bz - 128 : bz], 8 * i + 8, 1), up)
                down = jnp.where(mine, turn(window[p, :, 0:128], 8 * i, 1), down)
            pack[0, group] = up
            pack[1, group] = down
        for side in (0, 1):
            @pl.when(to_there[side])
            def _():
                z_copy(which, side).start()

    def z_finish(window, which):
        pack = packs_in[which]
        lane = cells(pack.shape[2:], 1)
        for side in (0, 1):
            @pl.when(from_there[side])
            def _():
                z_copy(which, side).wait_recv()

            @pl.when(jnp.logical_not(from_there[side]))
            def _():
                pack[side] = jnp.zeros(pack.shape[1:], jnp.float32)

            @pl.when(to_there[side])
            def _():
                z_copy(which, side).wait_send()

        for group, planes in enumerate(z_planes(which)):
            below = pack[0, group]
            above = pack[1, group]
            for i, p in enumerate(planes):
                window[p, :, bz : bz + 128] = jnp.where(
                    lane < 64, turn(above, -8 * i, 1), turn(below, -8 * i - 8, 1)
                )

    def fold_in(window):
        for p in z_planes(1)[0]:
            fine.r[p, :, 0:bz] = fold(window[p, :, 0:bz], eighth)

    def all_copy(source, target, which, peer, slot):
        return pltpu.make_async_remote_copy(
            src_ref=source,
            dst_ref=target.at[slot],
            send_sem=all_out.at[which, peer],
            recv_sem=all_in.at[which, slot],
            device_id=place(peer),
            device_id_type=MESH,
        )

    def all_start(source, target, which):
        target[me] = source[...]

        def step(j, carry):
            all_copy(source, target, which, (me + j) % count, me).start()
            return carry

        lax.fori_loop(1, count, step, 0)

    def all_wait(source, target, which):
        def step(j, carry):
            peer = (me + j) % count
            all_copy(source, target, which, peer, peer).wait_recv()
            all_copy(source, target, which, peer, me).wait_send()
            return carry

        lax.fori_loop(1, count, step, 0)

    half = bx // 2 * (by // 2)
    to_row, from_row = cells((half, bx * by), 0), cells((half, bx * by), 1)
    shrink = ones_where(
        (part_of(from_row, 2 * by) == part_of(to_row, by // 2))
        & (rest_of(from_row, by) >> 1 == rest_of(to_row, by // 2))
    )
    shrink_z = ones_where(cells((bz, bz // 2), 0) >> 1 == cells((bz, bz // 2), 1))

    def coarse_block(values):
        flat = pick(pick(shrink, values.reshape(bx * by, bz)), shrink_z) * 0.125
        return flat.reshape(half // 8, 8, bz // 2)

    row8 = cells((8, bz // 2), 0)

    def unpack(got, target):
        for jx in range(nx):
            for jy in range(0, ny, 2):
                for jz in range(nz):
                    slot = (jx * ny + jy) * nz + jz
                    for t in range(half // 8):
                        one, two = got[slot, t], got[slot + nz, t]
                        p = 1 + jx * (bx // 2) + 2 * t
                        at = (slice(jy * 4, jy * 4 + 8), slice(jz * bz // 2, (jz + 1) * bz // 2))
                        target[(p, *at)] = jnp.where(row8 < 4, one, turn(two, 4, 0))
                        target[(p + 1, *at)] = jnp.where(row8 < 4, turn(one, 4, 0), two)

    near_start(k_in, k_near, 0)
    near_start(b_in, b_near, 1)
    k_send[...] = coarse_block(k_in[...])
    k_near[bx : 2 * bx, 0:by, 0:bz] = k_in[...]
    b_near[bx : 2 * bx, 0:by, 0:bz] = b_in[...]
    edge = bx - reach - 1
    for ref in fine_refs:
        clear(ref, [edge, bx - 1, 2 * bx, 2 * bx + 1, 2 * bx + reach])
        clear(ref, (edge, bx))
        clear(ref, (2 * bx, 2 * bx + reach + 1))
    clear(d_wide, [2 * bx + reach])
    for ref in (mid.f, mid.g):
        clear(ref, [0, ref.shape[0] - 1])
    for ref in (low.f, low.g):
        clear(ref, [0, ref.shape[0] - 1])
    mx, my, mz = mid.k.shape[0] - 2, mid.k.shape[1], mid.k.shape[2]
    wide = bx + bx // 2
    mid_x = ix * (bx // 2) - bx // 2
    for q in range(wide):
        shape = (3 * by, mx * my)
        fine_row, mid_row = cells(shape, 0), cells(shape, 1)
        fine_y = iy * by + jnp.where(fine_row < 2 * by, fine_row, fine_row - 3 * by)
        target = (mid_x + q) * my + (fine_y >> 1)
        good = (fine_y >= 0) & (fine_y < ny * by) & (mid_x + q >= 0) & (mid_x + q < mx)
        rows_keep[q] = jnp.where((mid_row == target) & good, 1.0, 0.0)
    shape = (mz, bz + 128)
    fine_col = cells(shape, 1)
    fine_z = iz * bz + jnp.where(fine_col < bz + 64, fine_col, fine_col - (bz + 128))
    columns_keep[...] = ones_where((fine_z >> 1) == cells(shape, 0))
    near_wait(k_in, k_near, 0)
    z_start(k_near, 0)
    near_wait(b_in, b_near, 1)
    fold_in(b_near)
    z_start(fine.r, 1)
    all_start(k_send, k_got, 0)
    z_finish(k_near, 0)

    def span(width):
        return (
            jnp.maximum(bx - width, bx - ix * bx),
            jnp.minimum(2 * bx + width, bx + (nx - ix) * bx),
        )

    plane = (2 * by, bz + 128)
    row, col = cells(plane, 0), cells(plane, 1)
    inside = (
        (row < by) | ((row < by + 4) & (iy + 1 < ny)) | ((row >= by + 4) & (iy > 0))
    ) & ((col < bz) | ((col < bz + 64) & (iz + 1 < nz)) | ((col >= bz + 64) & (iz > 0)))
    fine.diagonal(span(5), span(4), inside)
    z_finish(fine.r, 1)

    own = (slice(bx, 2 * bx), slice(0, by), slice(0, bz))
    centre, weights = chebyshev_coefs(DEGREE, smooth_low)
    fine.first_update(span(4), centre)
    x_out[...] = fine.d[own]
    for number in range(DEGREE):
        pair = weights[number] if number < DEGREE - 1 else None
        fine.apply(span(4 - number), span(3 - number), pair)
        if pair is not None:
            x_out[...] += fine.d[own]

    r_send[...] = fine.r[own]
    b_send[...] = coarse_block(r_send[...])
    all_start(b_send, b_got, 1)
    near_start(r_send, r_near, 2)
    r_near[own] = r_send[...]

    cx, cy, cz = mx // 2, my // 2, mz // 2
    mid_span, low_span = (1, mx + 1), (1, cx + 1)
    all_wait(k_send, k_got, 0)
    unpack(k_got, mid.k)
    mid.diagonal(mid_span, mid_span, None)
    big, small = cells((cx * cy, mx * my), 1), cells((cx * cy, mx * my), 0)
    join = ones_where(
        (part_of(big, 2 * my) == part_of(small, cy)) & (rest_of(big, my) >> 1 == rest_of(small, cy))
    )
    join_z = ones_where(cells((mz, cz), 0) >> 1 == cells((mz, cz), 1))

    def to_low(values):
        flat = pick(join, pick(values.reshape(mx * my, mz), join_z)) * 0.125
        return flat.reshape(cx, cy, cz)

    low.k[1 : cx + 1] = to_low(mid.k[1 : mx + 1])
    low.diagonal(low_span, low_span, None)

    all_wait(b_send, b_got, 1)
    unpack(b_got, b_mid)
    mid.r[1 : mx + 1] = b_mid[1 : mx + 1]
    mid.first_update(mid_span, centre)
    x_mid[...] = mid.d[1 : mx + 1]
    for number in range(DEGREE):
        pair = weights[number] if number < DEGREE - 1 else None
        mid.apply(mid_span, mid_span, pair)
        if pair is not None:
            x_mid[...] += mid.d[1 : mx + 1]

    near_wait(r_send, r_near, 2)
    fold_in(r_near)
    z_start(fine.r, 2)

    low.r[1 : cx + 1] = to_low(mid.r[1 : mx + 1])
    low_centre, low_weights = chebyshev_coefs(COARSE_DEGREE, coarse_low)
    low.first_update(low_span, low_centre)
    x_low[...] = low.d[1 : cx + 1]
    for pair in low_weights:
        low.apply(low_span, low_span, pair)
        x_low[...] += low.d[1 : cx + 1]

    big, small = cells((mx * my, cx * cy), 0), cells((mx * my, cx * cy), 1)
    spread = ones_where(
        (part_of(big, 2 * my) == part_of(small, cy)) & (rest_of(big, my) >> 1 == rest_of(small, cy))
    )
    spread_z = ones_where(cells((cz, mz), 0) == cells((cz, mz), 1) >> 1)
    fixed = pick(spread, pick(x_low[...].reshape(cx * cy, cz), spread_z))
    mid.d[1 : mx + 1] = x_mid[...] + fixed.reshape(mx, my, mz)
    mid.r[1 : mx + 1] = b_mid[1 : mx + 1]
    x_mid[...] = mid.d[1 : mx + 1]
    mid.apply(mid_span, mid_span, (0.0, 1.0 / centre))
    x_mid[...] += mid.d[1 : mx + 1]
    for pair in weights:
        mid.apply(mid_span, mid_span, pair)
        x_mid[...] += mid.d[1 : mx + 1]

    z_finish(fine.r, 2)
    rows = rows_keep[...].reshape(wide * 3 * by, mx * my).astype(jnp.bfloat16)
    fixed = pick(rows, pick(x_mid[...].reshape(mx * my, mz), columns_keep[...]))
    fixed = fixed.reshape(wide, 3 * by, bz + 128)
    for p in range(bx - reach, 2 * bx + reach):
        d_wide[p] = fixed[p // 2]
    x_out[...] += d_wide[own]
    fine.apply(span(5), span(4), (0.0, 1.0 / centre), True)
    x_out[...] += fine.d[own]
    for number in range(DEGREE):
        pair = weights[number] if number < DEGREE - 1 else None
        fine.apply(span(4 - number), span(3 - number), pair)
        if pair is not None:
            x_out[...] += fine.d[own]
    r_out[...] = fine.r[own]


def gathered(sizes, conductivity, source):
    (nx, ny, nz) = sizes
    (bx, by, bz) = conductivity.shape
    count = nx * ny * nz
    mid = (nx * bx // 2 + 2, ny * by // 2, nz * bz // 2)
    low = (nx * bx // 4 + 2, ny * by // 4, nz * bz // 4)
    window = (3 * bx, 3 * by, bz + 128)
    narrow = (3 * bx, 2 * by, bz + 128)
    kept = lambda shape: pltpu.VMEM(shape, jnp.float32)
    inner_mid = (mid[0] - 2, *mid[1:])
    sent = (bx * by // 32, 8, bz // 2)
    scratch = [kept(narrow)] * 8 + [kept(mid)] * 8 + [kept(low)] * 8
    scratch += [kept(inner_mid), kept(mid), kept((low[0] - 2, *low[1:]))]
    scratch += [kept(sent), kept(sent), kept((bx, by, bz))]
    scratch += [kept((count, *sent)), kept((count, *sent))]
    scratch += [kept(window)] * 4
    packs = [kept((2, 2, 3 * by, 128)), kept((2, 1, 2 * by, 128)), kept((2, 1, 2 * by, 128))]
    scratch += packs + packs
    dma = pltpu.SemaphoreType.DMA
    scratch += [dma((3, 9)), dma((3, 9)), dma((3, 2)), dma((3, 2)), dma((2, count)), dma((2, count))]
    scratch += [kept((bx + bx // 2, 3 * by, inner_mid[0] * inner_mid[1]))]
    scratch += [pltpu.VMEM((inner_mid[2], bz + 128), jnp.bfloat16)]
    shape = jax.ShapeDtypeStruct((bx, by, bz), jnp.float32)
    vmem = pl.BlockSpec(memory_space=pltpu.VMEM)
    return pl.pallas_call(
        functools.partial(kernel, sizes, (bx, by, bz)),
        out_shape=(shape, shape),
        in_specs=[vmem, vmem],
        out_specs=(vmem, vmem),
        scratch_shapes=scratch,
        compiler_params=pltpu.CompilerParams(
            collective_id=0, has_side_effects=True, vmem_limit_bytes=48 * 1024 * 1024
        ),
    )(conductivity, source)


def plan(conductivity, source):
    sizes = tuple(lax.axis_size(axis) for axis in ("gx", "gy", "gz"))
    (bx, by, bz) = conductivity.shape
    count = sizes[0] * sizes[1] * sizes[2]
    fits = bx == 8 and by == 8 and bz % 256 == 0 and sizes[1] % 2 == 0
    if fits and count > 1 and count * bx * by * bz // 8 * 4 * 16 <= 16 * 1024 * 1024:
        return gathered(sizes, conductivity, source)
    return body(conductivity, source)


def solution(mesh):
    in_specs = (P("gx", "gy", "gz"), P("gx", "gy", "gz"))
    out_specs = (P("gx", "gy", "gz"), P("gx", "gy", "gz"))
    return jax.shard_map(plan, mesh=mesh, in_specs=in_specs, out_specs=out_specs, check_vma=False)
```
